32 devices in a mesh: dp: 2 (over x), tp: 4 (over z), sp: 4 (over y, core).
Axes of the slice: x: 2, y: 2, z: 4, core: 2. Of those that a mesh axis runs over, the one named last changes fastest.
Arguments:
- x_in: bfloat16 [131072, 192], P(('dp', 'sp')), parts along dimension 0
- grad_y: bfloat16 [131072, 192], P(('dp', 'sp')), parts along dimension 0
- w_qkv: bfloat16 [192, 3, 192], P(None, None, 'tp')
- w_out: bfloat16 [192, 192], P('tp')
- ln_gamma: float32 [192], replicated
- ln_beta: float32 [192], replicated
- temperature: float32 [4], replicated
Outputs:
- output 1: bfloat16 [131072, 192], P(('dp', 'sp')), parts along dimension 0
- output 2: bfloat16 [131072, 192], P(('dp', 'sp')), parts along dimension 0
- output 3: float32 [384, 3, 192], P(('dp', 'sp'), None, 'tp'), parts along dimension 0
- output 4: float32 [384, 192], P(('dp', 'tp', 'sp')), parts along dimension 0
- output 5: float32 [384], P('dp'), parts along dimension 0
- output 6: float32 [384], P('dp'), parts along dimension 0
- output 7: float32 [8], P('dp'), parts along dimension 0
There are 2 independent parts. The reference program is written for one: setup_inputs(seed, part) draws one part's arguments, and reference() takes and returns one part's arrays. A program takes and returns all parts, laid end to end along the dimension named above; an argument that names none is the same for every part.
All inputs are finite; a program needn't handle non-finite values.
Results may differ from the reference program's by a relative error of at most 0.001.
Values are sent between devices in bfloat16 or wider.
A program may use at most 1 GiB of HBM per device.

```python
import jax
import jax.numpy as jnp
from jax import lax

MODEL_DIM = 192
NUM_HEADS = 4
NUM_TOKENS = 65536
NUM_REGIONS = 8
HEAD_DIM = MODEL_DIM // NUM_HEADS
LN_EPS = 1e-6


def setup_inputs(seed: int = 0, part: int = 0) -> dict:
    part_key = jax.random.fold_in(jax.random.key(seed), part)
    key_noise, key_offset, key_grad, key_goffset = jax.random.split(part_key, 4)
    key_wqkv, key_wout, key_gamma, key_beta, key_temp = jax.random.split(jax.random.key(seed + 1), 5)
    rows_per_region = NUM_TOKENS // NUM_REGIONS
    w_scale = MODEL_DIM ** -0.5
    offsets = jax.random.normal(key_offset, (NUM_REGIONS, MODEL_DIM), jnp.float32)
    x_vals = jax.random.normal(key_noise, (NUM_TOKENS, MODEL_DIM), jnp.float32) + jnp.repeat(offsets, rows_per_region, axis=0)
    grad_offsets = 0.5 * jax.random.normal(key_goffset, (NUM_REGIONS, MODEL_DIM), jnp.float32)
    grad_vals = jax.random.normal(key_grad, (NUM_TOKENS, MODEL_DIM), jnp.float32) + jnp.repeat(grad_offsets, rows_per_region, axis=0)
    w_qkv = jax.random.normal(key_wqkv, (MODEL_DIM, 3, MODEL_DIM), jnp.float32) * w_scale
    w_out = jax.random.normal(key_wout, (MODEL_DIM, MODEL_DIM), jnp.float32) * w_scale
    ln_gamma = 1.0 + 0.3 * jax.random.normal(key_gamma, (MODEL_DIM,), jnp.float32)
    ln_beta = 0.3 * jax.random.normal(key_beta, (MODEL_DIM,), jnp.float32)
    temperature = jax.random.uniform(key_temp, (NUM_HEADS,), jnp.float32, 2.0, 4.0)
    return {"x_in": x_vals.astype(jnp.bfloat16), "grad_y": grad_vals.astype(jnp.bfloat16), "w_qkv": w_qkv.astype(jnp.bfloat16), "w_out": w_out.astype(jnp.bfloat16), "ln_gamma": ln_gamma, "ln_beta": ln_beta, "temperature": temperature}


def head_pass(operands):
    q_head, k_head, v_head, dout_head, temp_one = operands
    gram_mat = jnp.dot(q_head.T, k_head, preferred_element_type=jnp.float32)
    q_sq = jnp.sum(jnp.square(q_head.astype(jnp.float32)), axis=0)
    k_sq = jnp.sum(jnp.square(k_head.astype(jnp.float32)), axis=0)
    norm_prod = jnp.sqrt(q_sq)[:, None] * jnp.sqrt(k_sq)[None, :]
    gram_n = gram_mat / norm_prod
    attn_prob = jax.nn.softmax(temp_one * gram_n, axis=-1)
    attn_bf = attn_prob.astype(jnp.bfloat16)
    out_head = jnp.dot(v_head, attn_bf.T, preferred_element_type=jnp.float32).astype(jnp.bfloat16)
    d_attn = jnp.dot(dout_head.T, v_head, preferred_element_type=jnp.float32)
    dv_head = jnp.dot(dout_head, attn_bf, preferred_element_type=jnp.float32).astype(jnp.bfloat16)
    d_logit = attn_prob * (d_attn - jnp.sum(attn_prob * d_attn, axis=-1, keepdims=True))
    temp_grad = jnp.sum(d_logit * gram_n)
    grad_sn = temp_one * d_logit
    d_gram = (grad_sn / norm_prod).astype(jnp.bfloat16)
    prod_sn = grad_sn * gram_n
    q_coef = -jnp.sum(prod_sn, axis=1) / q_sq
    k_coef = -jnp.sum(prod_sn, axis=0) / k_sq
    dq_head = (jnp.dot(k_head, d_gram.T, preferred_element_type=jnp.float32) + q_head.astype(jnp.float32) * q_coef[None, :]).astype(jnp.bfloat16)
    dk_head = (jnp.dot(q_head, d_gram, preferred_element_type=jnp.float32) + k_head.astype(jnp.float32) * k_coef[None, :]).astype(jnp.bfloat16)
    return out_head, dq_head, dk_head, dv_head, temp_grad


def reference(x_in, grad_y, w_qkv, w_out, ln_gamma, ln_beta, temperature):
    x_float = x_in.astype(jnp.float32)
    centered = x_float - jnp.mean(x_float, axis=1, keepdims=True)
    inv_std = lax.rsqrt(jnp.mean(centered * centered, axis=1, keepdims=True) + LN_EPS)
    x_hat = centered * inv_std
    u_act = (x_hat * ln_gamma + ln_beta).astype(jnp.bfloat16)
    w_flat = w_qkv.reshape(MODEL_DIM, 3 * MODEL_DIM)
    qkv_act = jnp.dot(u_act, w_flat, preferred_element_type=jnp.float32).astype(jnp.bfloat16)
    qkv_heads = qkv_act.reshape(NUM_TOKENS, 3, NUM_HEADS, HEAD_DIM).transpose(1, 2, 0, 3)
    dout_act = jnp.dot(grad_y, w_out.T, preferred_element_type=jnp.float32).astype(jnp.bfloat16)
    dout_heads = dout_act.reshape(NUM_TOKENS, NUM_HEADS, HEAD_DIM).transpose(1, 0, 2)
    out_heads, dq_heads, dk_heads, dv_heads, grad_temp = lax.map(head_pass, (qkv_heads[0], qkv_heads[1], qkv_heads[2], dout_heads, temperature))
    out_act = out_heads.transpose(1, 0, 2).reshape(NUM_TOKENS, MODEL_DIM)
    y_out = (x_float + jnp.dot(out_act, w_out, preferred_element_type=jnp.float32)).astype(jnp.bfloat16)
    grad_wout = jnp.dot(out_act.T, grad_y, preferred_element_type=jnp.float32)
    dqkv_act = jnp.stack([dq_heads, dk_heads, dv_heads], axis=0).transpose(2, 0, 1, 3).reshape(NUM_TOKENS, 3 * MODEL_DIM)
    grad_wqkv = jnp.dot(u_act.T, dqkv_act, preferred_element_type=jnp.float32).reshape(MODEL_DIM, 3, MODEL_DIM)
    grad_u = jnp.dot(dqkv_act, w_flat.T, preferred_element_type=jnp.float32)
    grad_gamma = jnp.sum(grad_u * x_hat, axis=0)
    grad_beta = jnp.sum(grad_u, axis=0)
    grad_xhat = grad_u * ln_gamma
    grad_ln = inv_std * (grad_xhat - jnp.mean(grad_xhat, axis=1, keepdims=True) - x_hat * jnp.mean(grad_xhat * x_hat, axis=1, keepdims=True))
    grad_x = (grad_y.astype(jnp.float32) + grad_ln).astype(jnp.bfloat16)
    return y_out, grad_x, grad_wqkv, grad_wout, grad_gamma, grad_beta, grad_temp
```

```python
import jax
import jax.numpy as jnp
from jax import lax
from jax.experimental import pallas as pl
from jax.experimental.pallas import tpu as pltpu
from jax.sharding import PartitionSpec as P

LN_EPS = 1e-6
D = 192
NH = 4
HD = 48
F32 = jnp.float32
BF16 = jnp.bfloat16
MESH = pl.DeviceIdType.MESH
BLK1 = 2048
BLK2 = 2048
SUB = 1024


def dot_nn(a, b):
    return lax.dot_general(a, b, (((1,), (0,)), ((), ())), preferred_element_type=F32)


def dot_nt(a, b):
    return lax.dot_general(a, b, (((1,), (1,)), ((), ())), preferred_element_type=F32)


def norm_cols(x_cols):
    xf = x_cols.astype(F32)
    cen = xf - jnp.sum(xf, axis=0, keepdims=True) * (1.0 / D)
    inv = lax.rsqrt(jnp.sum(cen * cen, axis=0, keepdims=True) * (1.0 / D) + LN_EPS)
    return xf, cen * inv, inv


def fold_lanes(val):
    out = val[:, 0:128]
    for c in range(128, val.shape[1], 128):
        out = out + val[:, c:c + 128]
    return out


def lane_iota(shape):
    return lax.broadcasted_iota(jnp.int32, shape, len(shape) - 1)


def enter(axis, me):
    barrier = pltpu.get_barrier_semaphore()
    for d in range(1, 4):
        pl.semaphore_signal(barrier, inc=1, device_id={axis: lax.rem(me + d, 4)}, device_id_type=MESH)


def remote(src, dst, sems, d, axis, peer):
    return pltpu.make_async_remote_copy(
        src_ref=src, dst_ref=dst, send_sem=sems[0].at[d - 1], recv_sem=sems[1].at[d - 1],
        device_id={axis: peer}, device_id_type=MESH)


def pad_lanes(val, lanes):
    return jnp.concatenate([val, jnp.zeros((val.shape[0], lanes - val.shape[1]), val.dtype)], axis=1)


def pad_rows(val, rows):
    return jnp.concatenate([val, jnp.zeros((rows - val.shape[0], val.shape[1]), val.dtype)], axis=0)


def as_column(row_1d):
    row = jnp.broadcast_to(row_1d.reshape(1, D), (128, D))
    return row.T


def state_kernel(x_hbm, g_hbm, wqkv_ref, wo_ref, gam_ref, bet_ref, temp_ref,
                 wt_out, w_out, mats_ref, vecs_ref, temp_out,
                 xs, gs, wbuf, gram_acc, da_acc, sq_acc, pay_buf, st_send, st_buf, vec_send, vec_buf,
                 in_sems, w_ssem, w_rsem, o_ssem, o_rsem, p_ssem, p_rsem, s_ssem, s_rsem, v_ssem, v_rsem):
    t = lax.axis_index("tp")
    s = lax.axis_index("sp")
    n_load = xs.shape[1] // BLK1

    def loads(c):
        cols = pl.ds(pl.multiple_of(c * BLK1, BLK1), BLK1)
        return (pltpu.make_async_copy(x_hbm.at[:, cols], xs.at[:, cols], in_sems.at[0, c]),
                pltpu.make_async_copy(g_hbm.at[:, cols], gs.at[:, cols], in_sems.at[1, c]))

    for c in range(n_load):
        for cp in loads(c):
            cp.start()
    enter("tp", t)
    enter("sp", s)
    pl.semaphore_wait(pltpu.get_barrier_semaphore(), 6)

    def w_copies(d):
        peer = lax.rem(t + d, 4)
        return (remote(wqkv_ref, wbuf.at[t, pl.ds(0, 3)], (w_ssem, w_rsem), d, "tp", peer),
                remote(wo_ref, wbuf.at[t, 3], (o_ssem, o_rsem), d, "tp", peer))

    for d in range(1, 4):
        for cp in w_copies(d):
            cp.start()
    wbuf[pl.ds(t, 1), 0:3] = wqkv_ref[...][None]
    wbuf[pl.ds(t, 1), 3] = wo_ref[...][None]
    gram_acc[...] = jnp.zeros_like(gram_acc)
    da_acc[...] = jnp.zeros_like(da_acc)
    sq_acc[...] = jnp.zeros_like(sq_acc)
    vecs_ref[2] = as_column(gam_ref[...])
    vecs_ref[3] = as_column(bet_ref[...])
    gamma = vecs_ref[2, :, 0:1]
    beta = vecs_ref[3, :, 0:1]
    w_own = wqkv_ref[...].reshape(3 * HD, D)

    def body(c, carry):
        for cp in loads(c):
            cp.wait()
        cols = pl.ds(pl.multiple_of(c * BLK1, BLK1), BLK1)
        _, xh, _ = norm_cols(xs[:, cols])
        u = (xh * gamma + beta).astype(BF16)
        qkv = dot_nn(w_own, u).astype(BF16)
        do = dot_nn(wo_ref[...], gs[:, cols]).astype(BF16)
        q, k, v = qkv[0:HD], qkv[HD:2 * HD], qkv[2 * HD:3 * HD]
        gram_acc[...] += dot_nt(q, k)
        da_acc[...] += dot_nt(do, v)
        qf = q.astype(F32)
        kf = k.astype(F32)
        sq_acc[0] += fold_lanes(qf * qf)
        sq_acc[1] += fold_lanes(kf * kf)
        return carry

    lax.fori_loop(0, n_load, body, 0)

    lane = lane_iota((HD, 128))
    msg = jnp.where(lane < 64, pad_lanes(gram_acc[...], 128), pltpu.roll(pad_lanes(da_acc[...], 128), 64, 1))
    asq = jnp.sum(sq_acc[0], axis=1, keepdims=True)
    bsq = jnp.sum(sq_acc[1], axis=1, keepdims=True)
    msg = jnp.where(lane == 112, asq, jnp.where(lane == 113, bsq, msg))
    pay_buf[pl.ds(s, 1)] = msg[None]

    def p_copy(d):
        return remote(pay_buf.at[s], pay_buf.at[s], (p_ssem, p_rsem), d, "sp", lax.rem(s + d, 4))

    for d in range(1, 4):
        p_copy(d).start()
    for d in range(1, 4):
        for cp in w_copies(d):
            cp.wait()
    for e in range(4):
        wt_full = wbuf[:, e].reshape(D, D)
        wt_out[e * D:(e + 1) * D] = wt_full
        w_out[e] = wt_full.T
    for d in range(1, 4):
        p_copy(d).wait()

    tot = (pay_buf[0] + pay_buf[1]) + (pay_buf[2] + pay_buf[3])
    row = lax.broadcasted_iota(jnp.int32, (HD, 128), 0)
    live = lane < HD
    eye = lane == row
    temp = temp_ref[t]
    gm = jnp.where(live, tot, 0.0)
    da = jnp.where(live, pltpu.roll(tot, 64, 1), 0.0)
    a_col = tot[:, 112:113]
    b_col = tot[:, 113:114]
    b_row = jnp.sum(jnp.where(eye, b_col, 0.0), axis=0, keepdims=True)
    b_row = jnp.where(lane_iota((1, 128)) < HD, b_row, 1.0)
    norm = jnp.sqrt(a_col) * jnp.sqrt(b_row)
    sn = gm / norm
    logit = jnp.where(live, temp * sn, -1e30)
    ex = jnp.where(live, jnp.exp(logit - jnp.max(logit, axis=1, keepdims=True)), 0.0)
    attn = ex / jnp.sum(ex, axis=1, keepdims=True)
    dl = attn * (da - jnp.sum(attn * da, axis=1, keepdims=True))
    dtau = jnp.sum(jnp.sum(dl * sn, axis=1, keepdims=True), axis=0, keepdims=True)
    grad_sn = temp * dl
    dg = grad_sn / norm
    prod = grad_sn * sn
    cq_col = -jnp.sum(prod, axis=1, keepdims=True) / a_col
    ck_row = -jnp.sum(prod, axis=0, keepdims=True) / b_row
    cq_row = jnp.sum(jnp.where(eye, cq_col, 0.0), axis=0, keepdims=True)
    row8 = lax.broadcasted_iota(jnp.int32, (8, 128), 0)
    vec_send[...] = jnp.where(row8 == 0, cq_row, jnp.where(row8 == 1, ck_row, jnp.where(row8 == 2, dtau, 0.0)))
    for half, val in enumerate((attn, dg)):
        flip = pltpu.roll(pad_rows(val, 128).T[0:HD], 64, 1)
        st_send[:, 128 * half:128 * half + 128] = jnp.where(lane < 64, val, flip).astype(BF16)

    def s_copies(d):
        peer = lax.rem(t + d, 4)
        return (remote(st_send, st_buf.at[t], (s_ssem, s_rsem), d, "tp", peer),
                remote(vec_send, vec_buf.at[t], (v_ssem, v_rsem), d, "tp", peer))

    for d in range(1, 4):
        for cp in s_copies(d):
            cp.start()
    st_buf[pl.ds(t, 1)] = st_send[...][None]
    vec_buf[pl.ds(t, 1)] = vec_send[...][None]
    for d in range(1, 4):
        for cp in s_copies(d):
            cp.wait()
    lane2 = lane_iota((HD, 256))
    vec_t = pad_rows(vec_buf[...].reshape(32, 128), 128).T
    for h in range(NH):
        wide = st_buf[h].astype(F32)
        here = (lane2 >= HD * h) & (lane2 < HD * h + HD)
        for j in range(4):
            shift = (HD * h - 64 * j) % 256
            moved = pltpu.roll(wide, shift, 1) if shift else wide
            mats_ref[j, HD * h:HD * h + HD] = jnp.where(here, moved, 0.0)[:, :D].astype(BF16)
        for j in range(2):
            vecs_ref[j, HD * h:HD * h + HD] = jnp.broadcast_to(vec_t[0:HD, 8 * h + j:8 * h + j + 1], (HD, 128))
    lane8 = lane_iota((8, 128))
    taus = jnp.zeros((8, 128), F32)
    for h in range(NH):
        taus = jnp.where(lane8 == h, vec_buf[h, 2:3, 0:1], taus)
    temp_out[...] = taus


def col_pass(xb, gb, wt_ref, w_ref, mats_ref, vecs_ref):
    cq, ck, gamma, beta = [vecs_ref[j, :, 0:1] for j in range(4)]
    xf, xh, inv = norm_cols(xb)
    u = (xh * gamma + beta).astype(BF16)
    q = dot_nn(wt_ref[0:D], u).astype(BF16)
    k = dot_nn(wt_ref[D:2 * D], u).astype(BF16)
    v = dot_nn(wt_ref[2 * D:3 * D], u).astype(BF16)
    do = dot_nn(wt_ref[3 * D:4 * D], gb).astype(BF16)
    o = dot_nn(mats_ref[0], v).astype(BF16)
    y = (xf + dot_nn(w_ref[3], o)).astype(BF16)
    dv = dot_nn(mats_ref[1], do).astype(BF16)
    dq = (dot_nn(mats_ref[2], k) + q.astype(F32) * cq).astype(BF16)
    dk = (dot_nn(mats_ref[3], q) + k.astype(F32) * ck).astype(BF16)
    du = dot_nn(w_ref[0], dq) + dot_nn(w_ref[1], dk) + dot_nn(w_ref[2], dv)
    gx = du * gamma
    m1 = jnp.sum(gx, axis=0, keepdims=True) * (1.0 / D)
    m2 = jnp.sum(gx * xh, axis=0, keepdims=True) * (1.0 / D)
    dx = (gb.astype(F32) + inv * (gx - m1 - xh * m2)).astype(BF16)
    return y, dx, xh, u, o, du, (dq, dk, dv)


def rows_kernel(tp_ref, x_ref, g_ref, wt_ref, w_ref, mats_ref, vecs_ref, y_ref, dx_ref, send_ref,
                acc_w, acc_v, r_s):
    i = pl.program_id(0)
    own = pl.ds(pl.multiple_of(tp_ref[0] * HD, 16), HD)

    @pl.when(i == 0)
    def _():
        acc_w[...] = jnp.zeros_like(acc_w)
        acc_v[...] = jnp.zeros_like(acc_v)

    for lo in range(0, BLK2, SUB):
        sub = slice(lo, lo + SUB)
        gb = g_ref[:, sub]
        y, dx, xh, u, o, du, r = col_pass(x_ref[:, sub], gb, wt_ref, w_ref, mats_ref, vecs_ref)
        y_ref[:, sub] = y
        dx_ref[:, sub] = dx
        for e in range(3):
            r_s[e] = r[e]
        r_s[3] = o
        acc_w[0:3 * HD] += dot_nt(r_s[0:3, own].reshape(3 * HD, SUB), u)
        acc_w[3 * HD:4 * HD] += dot_nt(r_s[3, own], gb)
        acc_v[0] += fold_lanes(du * xh)
        acc_v[1] += fold_lanes(du)

    @pl.when(i == pl.num_programs(0) - 1)
    def _():
        lane = lane_iota((D, 128))
        dgam = jnp.sum(acc_v[0], axis=1, keepdims=True)
        dbet = jnp.sum(acc_v[1], axis=1, keepdims=True)
        both = jnp.where(lane == 0, dgam, jnp.where(lane == 1, dbet, 0.0))
        dvec = pad_lanes(both.T[0:8], 256)
        wide = [pad_lanes(acc_w[e * HD:(e + 1) * HD], 256) for e in range(4)]
        lane2 = lane_iota((HD, 256))
        for sp in range(4):
            cut = [pltpu.roll(wide[e], (256 + 64 * e - HD * sp) % 256, 1) if 64 * e != HD * sp else wide[e]
                   for e in range(3)]
            msg = jnp.where(lane2 < 64, cut[0], jnp.where(lane2 < 128, cut[1], cut[2]))
            send_ref[sp, 0:HD] = msg
            moved = pltpu.roll(wide[3], HD - 12 * sp, 0) if sp else wide[3]
            send_ref[sp, HD:HD + 16] = moved[0:16]
            send_ref[sp, HD + 16:HD + 24] = dvec


def reduce_kernel(send_ref, out_ref, recv, ssem, rsem):
    s = lax.axis_index("sp")
    enter("sp", s)
    pl.semaphore_wait(pltpu.get_barrier_semaphore(), 3)

    def copy(d):
        peer = lax.rem(s + d, 4)
        return remote(send_ref.at[peer], recv.at[s], (ssem, rsem), d, "sp", peer)

    for d in range(1, 4):
        copy(d).start()
    recv[pl.ds(s, 1)] = send_ref[pl.ds(s, 1)]
    for d in range(1, 4):
        copy(d).wait()
    out_ref[...] = (recv[0] + recv[1]) + (recv[2] + recv[3])


def finish_kernel(res_ref, tau_ref, gw_ref, gwo_ref, gg_ref, gb_ref, gt_ref):
    full = pad_rows(res_ref[0:HD], 128)
    both = full[:, 0:128].T
    gw_ref[0] = both[0:HD, 0:HD]
    gw_ref[1] = both[64:64 + HD, 0:HD]
    gw_ref[2] = full[:, 128:256].T[0:HD, 0:HD]
    gwo_ref[...] = res_ref[HD:HD + 12, 0:D]
    gg_ref[...] = res_ref[HD + 16, 0:D]
    gb_ref[...] = res_ref[HD + 17, 0:D]
    gt_ref[...] = tau_ref[0, 0:NH]


def solution(mesh):
    row_spec = P(("dp", "sp"), None)

    def local_step(x_blk, grad_blk, w_qkv, w_out, ln_gamma, ln_beta, temperature):
        tokens = x_blk.shape[0]
        x_t = x_blk.T
        g_t = grad_blk.T
        wqkv_t = jnp.transpose(w_qkv, (1, 2, 0))
        vmem = pl.BlockSpec(memory_space=pltpu.VMEM)
        hbm = pl.BlockSpec(memory_space=pl.ANY)
        dma = pltpu.SemaphoreType.DMA
        sds = jax.ShapeDtypeStruct
        wt_full, w_full, mats, vecs, taus = pl.pallas_call(
            state_kernel,
            name="state_kernel",
            out_shape=(sds((4 * D, D), BF16), sds((4, D, D), BF16), sds((4, D, D), BF16), sds((4, D, 128), F32),
                       sds((8, 128), F32)),
            in_specs=[hbm, hbm, vmem, vmem, vmem, vmem, pl.BlockSpec(memory_space=pltpu.SMEM)],
            out_specs=(vmem,) * 5,
            scratch_shapes=[
                pltpu.VMEM((D, tokens), BF16), pltpu.VMEM((D, tokens), BF16),
                pltpu.VMEM((4, 4, HD, D), BF16),
                pltpu.VMEM((HD, HD), F32), pltpu.VMEM((HD, HD), F32), pltpu.VMEM((2, HD, 128), F32),
                pltpu.VMEM((4, HD, 128), F32), pltpu.VMEM((HD, 256), BF16), pltpu.VMEM((4, HD, 256), BF16),
                pltpu.VMEM((8, 128), F32), pltpu.VMEM((4, 8, 128), F32),
                dma((2, tokens // BLK1)), dma((3,)), dma((3,)), dma((3,)), dma((3,)), dma((3,)), dma((3,)),
                dma((3,)), dma((3,)), dma((3,)), dma((3,)),
            ],
            compiler_params=pltpu.CompilerParams(collective_id=0, has_side_effects=True),
        )(x_t, g_t, wqkv_t, w_out, ln_gamma, ln_beta, temperature)

        nblk = tokens // BLK2
        tp_idx = lax.axis_index("tp").astype(jnp.int32).reshape(1)
        cols = pl.BlockSpec((D, BLK2), lambda i, st: (0, i))

        def whole(*shape):
            return pl.BlockSpec(shape, lambda i, st: (0,) * len(shape))

        y_t, dx_t, part = pl.pallas_call(
            rows_kernel,
            name="rows_kernel",
            out_shape=(sds((D, tokens), BF16), sds((D, tokens), BF16), sds((4, HD + 24, 256), F32)),
            grid_spec=pltpu.PrefetchScalarGridSpec(
                num_scalar_prefetch=1, grid=(nblk,),
                in_specs=[cols, cols, whole(4 * D, D), whole(4, D, D), whole(4, D, D), whole(4, D, 128)],
                out_specs=(cols, cols, whole(4, HD + 24, 256)),
                scratch_shapes=[pltpu.VMEM((4 * HD, D), F32), pltpu.VMEM((2, D, 128), F32),
                                pltpu.VMEM((4, D, SUB), BF16)]),
            compiler_params=pltpu.CompilerParams(dimension_semantics=("arbitrary",)),
        )(tp_idx, x_t, g_t, wt_full, w_full, mats, vecs)

        res = pl.pallas_call(
            reduce_kernel,
            name="reduce_kernel",
            out_shape=sds((HD + 24, 256), F32),
            in_specs=[vmem],
            out_specs=vmem,
            scratch_shapes=[pltpu.VMEM((4, HD + 24, 256), F32), dma((3,)), dma((3,))],
            compiler_params=pltpu.CompilerParams(collective_id=1, has_side_effects=True),
        )(part)
        gw, gwo, gg, gb, gt = pl.pallas_call(
            finish_kernel,
            name="finish_kernel",
            out_shape=(sds((3, HD, HD), F32), sds((12, D), F32), sds((D,), F32), sds((D,), F32), sds((NH,), F32)),
            in_specs=[vmem, vmem],
            out_specs=(vmem,) * 5,
        )(res, taus)
        return y_t.T, dx_t.T, jnp.transpose(gw, (1, 0, 2)), gwo, gg, gb, gt

    in_specs = (row_spec, row_spec, P(None, None, "tp"), P("tp", None), P(None), P(None), P(None))
    out_specs = (row_spec, row_spec, P(("dp", "sp"), None, "tp"), P(("dp", "tp", "sp"), None), P("dp"), P("dp"), P("dp"))
    return jax.shard_map(local_step, mesh=mesh, in_specs=in_specs, out_specs=out_specs, check_vma=False)
```
